32 devices in a mesh: lon: 8 (over z, y), lat: 4 (over x, core).
Axes of the slice: x: 2, y: 2, z: 4, core: 2. Of those that a mesh axis runs over, the one named last changes fastest.
Arguments:
- terrain_relief: float32 [1, 2688, 10752], P(None, 'lon', 'lat'), may hold values from -30 to 30
Outputs:
- smoothed: float32 [1, 2688, 10752], P(None, 'lon', 'lat')
- slope: float32 [1, 2688, 10752], P(None, 'lon', 'lat')
The draws below stay inside these ranges and needn't reach their ends.
All inputs are finite; a program needn't handle non-finite values.
Results may differ from the reference program's by a relative error of at most 0.0001.
Values sent between devices are 32-bit elements; how exact they have to be, the bound alone decides.
A program may use at most 64 MiB of HBM per device.

```python
import jax
import jax.numpy as jnp
from jax import lax

MEMBERS = 1
NLON = 2688
NLAT = 10752


def draw_terrain_relief(key, part):
    first_key, later_random_seed = jax.random.split(key, 2)
    grid_extent = (MEMBERS, NLON, NLAT)
    column = jnp.arange(NLON, dtype=jnp.float32)[None, :, None]
    trend = 1.0 + 2.0 * column / NLON
    factor = jnp.exp(jax.random.uniform(later_random_seed, grid_extent, jnp.float32, jnp.log(0.5), jnp.log(2.0)))
    noise = jnp.clip(jax.random.normal(first_key, grid_extent, jnp.float32), -4.0, 4.0)
    return (trend + 3.0 * factor * noise).astype(jnp.float32)


def setup_inputs(seed: int = 0) -> dict:
    keys = jax.random.split(jax.random.key(seed), 2)
    return {
        "terrain_relief": draw_terrain_relief(jax.random.fold_in(keys[1], 71), 0),
    }


def filter_pass(relief_surface):
    lat_count = relief_surface.shape[1]
    lon_sum = sum((jnp.roll(relief_surface, -offset, 0) for offset in range(-2, 3)))
    padded = jnp.pad(lon_sum, ((0, 0), (2, 2)))
    box_total = sum((padded[:, offset:offset + lat_count] for offset in range(5)))
    row_index = jnp.arange(lat_count, dtype=jnp.int32)
    counted = (jnp.minimum(row_index + 2, lat_count - 1) - jnp.maximum(row_index - 2, 0) + 1).astype(jnp.float32)
    final_output = box_total / (5.0 * counted)
    north_mean = jnp.mean(final_output[:, 0])
    south_mean = jnp.mean(final_output[:, lat_count - 1])
    final_output = final_output.at[:, 0].set(north_mean)
    final_output = final_output.at[:, lat_count - 1].set(south_mean)
    return final_output

def horn_slope(relief_surface):
    lat_count = relief_surface.shape[1]
    across = jnp.roll(relief_surface, -1, 0) - jnp.roll(relief_surface, 1, 0)
    padded_across = jnp.pad(across, ((0, 0), (1, 1)))
    east_west = padded_across[:, :-2] + 2.0 * padded_across[:, 1:-1] + padded_across[:, 2:]
    padded = jnp.pad(relief_surface, ((0, 0), (1, 1)))
    upward = padded[:, 2:] - padded[:, :-2]
    north_south = jnp.roll(upward, 1, 0) + 2.0 * upward + jnp.roll(upward, -1, 0)
    row_index = jnp.arange(lat_count, dtype=jnp.int32).astype(jnp.float32)
    latitude = jnp.pi * ((row_index + 0.5) / lat_count - 0.5)
    stretch = 1.0 / jnp.maximum(jnp.cos(latitude), 0.1)
    grad_x = east_west * stretch / 8.0
    grad_y = north_south / 8.0
    return jnp.sqrt(1.0 + grad_x * grad_x + grad_y * grad_y)

def sole_realization_case(relief_surface):
    for repetitions in range(2):
        relief_surface = filter_pass(relief_surface)
    return (relief_surface, horn_slope(relief_surface))

def reference(terrain_relief):
    return lax.map(sole_realization_case, terrain_relief)
```

```python
import functools

import jax
import jax.numpy as jnp
from jax import lax
from jax.experimental import pallas as pl
from jax.experimental.pallas import tpu as pltpu
from jax.sharding import PartitionSpec as P

LANES = 128
SUB = 8
PAD = 16


class Strip:
    def __init__(self, count, make):
        self.count, self.make = count, make
        self.values, self.rolled = {}, {}

    def __getitem__(self, block):
        block %= self.count
        if block not in self.values:
            self.values[block] = self.make(block)
        return self.values[block]

    def roll(self, block, shift):
        key = (block % self.count, shift)
        if key not in self.rolled:
            self.rolled[key] = pltpu.roll(self[block], (-shift) % LANES, 1)
        return self.rolled[key]

    def ahead(self, block, shift, lane):
        if shift > 0:
            return jnp.where(lane < LANES - shift, self.roll(block, shift), self.roll(block + 1, shift))
        return jnp.where(lane >= -shift, self.roll(block, shift), self.roll(block - 1, shift))


def box_strip(src, dst, row, blocks, total_blocks, lane, scale, extra):
    def lon_sum(b):
        rows = [src[b, pl.ds(row + d, SUB), :] for d in (-2, -1, 0, 1, 2)]
        return ((rows[0] + rows[1]) + (rows[3] + rows[4])) + rows[2]

    one = Strip(total_blocks, lon_sum)
    two = Strip(total_blocks, lambda b: one[b] + one.ahead(b, 1, lane))
    for b in blocks:
        total = (two[b] + two.ahead(b, -2, lane)) + one.ahead(b, 2, lane)
        if b in scale:
            value = total * scale[b] + extra[b]
        else:
            value = total * (1.0 / 25.0)
        dst[b, pl.ds(row, SUB), :] = value
        yield b, value


def run(strip):
    for _ in strip:
        pass


def edge_rows(blocks, rows_here, start, lane):
    inner = blocks - 1
    return {
        0: start + lane,
        inner - 1: start + rows_here - LANES + lane,
        inner: jnp.where(lane < LANES // 2, start + rows_here + lane, start - LANES + lane),
    }


def edge_factors(blocks, rows_here, total_rows, start, lane, mean):
    scale, extra = {}, {}
    for b, row in edge_rows(blocks, rows_here, start, lane).items():
        low = jnp.maximum(row - 2, 0)
        high = jnp.minimum(row + 2, total_rows - 1)
        counted = jnp.maximum(high - low + 1, 1).astype(jnp.float32)
        polar = (row == 0) | (row == total_rows - 1)
        inside = (row > 0) & (row < total_rows - 1)
        scale[b] = jnp.where(inside, 1.0 / (5.0 * counted), 0.0)
        extra[b] = jnp.where(polar, mean, 0.0)
    return scale, extra


def first_kernel(n_lon, n_lat, cols, rows_here, x_hbm, z1, means, x, e, gat, in_sem, send, recv, gsend, grecv):
    inner = rows_here // LANES
    blocks = inner + 1
    lon, lat = lax.axis_index("lon"), lax.axis_index("lat")
    total_rows = rows_here * n_lat
    east, west = lax.rem(lon + 1, n_lon), lax.rem(lon + n_lon - 1, n_lon)
    has_north, has_south = lat > 0, lat < n_lat - 1
    pole = jnp.logical_not(has_north & has_south)
    lane = lax.broadcasted_iota(jnp.int32, (SUB, LANES), 1)

    loads = [
        pltpu.make_async_copy(
            x_hbm.at[0, :, pl.ds(b * LANES, LANES)], x.at[b, pl.ds(PAD, cols), :], in_sem.at[b]
        )
        for b in range(inner)
    ]
    for b in [0, inner - 1] + list(range(1, inner - 1)):
        loads[b].start()

    barrier = pltpu.get_barrier_semaphore()

    def greet(to_lon, to_lat):
        pl.semaphore_signal(
            barrier, inc=1, device_id=(to_lon, to_lat), device_id_type=pl.DeviceIdType.MESH
        )

    greet(east, lat)
    greet(west, lat)

    @pl.when(has_north)
    def _():
        for to_lon in (lon, east, west):
            greet(to_lon, lat - 1)

    @pl.when(has_south)
    def _():
        for to_lon in (lon, east, west):
            greet(to_lon, lat + 1)

    @pl.when(pole)
    def _():
        def one(d, carry):
            greet(lax.rem(lon + d, n_lon), lat)
            return carry

        lax.fori_loop(2, n_lon - 1, one, 0)

    def remote(src, dst, i, to_lon, to_lat):
        return pltpu.make_async_remote_copy(
            src_ref=src,
            dst_ref=dst,
            send_sem=send.at[i],
            recv_sem=recv.at[i],
            device_id=(to_lon, to_lat),
            device_id_type=pl.DeviceIdType.MESH,
        )

    own = pl.ds(PAD, cols)
    head, tail = pl.ds(PAD, SUB), pl.ds(PAD + cols - SUB, SUB)
    before, after = pl.ds(PAD - SUB, SUB), pl.ds(PAD + cols, SUB)
    band = pl.ds(0, inner)
    last = inner - 1
    lon_copies = [
        remote(x.at[band, tail, :], x.at[band, before, :], 0, east, lat),
        remote(x.at[band, head, :], x.at[band, after, :], 1, west, lat),
    ]
    south_copies = [
        remote(x.at[last, own, :], e.at[0, own, :], 2, lon, lat + 1),
        remote(x.at[last, tail, :], e.at[0, before, :], 3, east, lat + 1),
        remote(x.at[last, head, :], e.at[0, after, :], 4, west, lat + 1),
    ]
    north_copies = [
        remote(x.at[0, own, :], e.at[1, own, :], 5, lon, lat - 1),
        remote(x.at[0, tail, :], e.at[1, before, :], 6, east, lat - 1),
        remote(x.at[0, head, :], e.at[1, after, :], 7, west, lat - 1),
    ]

    def gather_copy(d):
        return pltpu.make_async_remote_copy(
            src_ref=gat.at[0],
            dst_ref=gat.at[d],
            send_sem=gsend.at[d],
            recv_sem=grecv.at[d],
            device_id=(lax.rem(lon + d, n_lon), lat),
            device_id_type=pl.DeviceIdType.MESH,
        )

    loads[0].wait()
    loads[last].wait()

    def partial_sum(block):
        def one(t, total):
            return total + x[block, pl.ds(pl.multiple_of(PAD + t * SUB, SUB), SUB), :]

        gat[0] = lax.fori_loop(0, cols // SUB, one, jnp.zeros((SUB, LANES), jnp.float32), unroll=True)

    pl.when(lat == 0)(lambda: partial_sum(0))
    pl.when(lat == n_lat - 1)(lambda: partial_sum(last))

    signals = 2 + 3 * has_north.astype(jnp.int32) + 3 * has_south.astype(jnp.int32)
    signals = signals + (n_lon - 3) * pole.astype(jnp.int32)
    pl.semaphore_wait(barrier, signals)

    @pl.when(has_south)
    def _():
        for copy in south_copies:
            copy.start()

    @pl.when(has_north)
    def _():
        for copy in north_copies:
            copy.start()

    for b in range(1, last):
        loads[b].wait()
    for copy in lon_copies:
        copy.start()

    def each_gather(act):
        @pl.when(pole)
        def _():
            def one(d, carry):
                act(gather_copy(d))
                return carry

            lax.fori_loop(1, n_lon, one, 0)

    each_gather(lambda copy: copy.start())

    def clear(side):
        e[side] = jnp.zeros(e.shape[1:], jnp.float32)

    pl.when(jnp.logical_not(has_north))(lambda: clear(0))
    pl.when(jnp.logical_not(has_south))(lambda: clear(1))

    strips = cols // SUB

    def row_of(t):
        return pl.multiple_of(PAD + t * SUB, SUB)

    def interior(t, carry):
        run(box_strip(x, z1, row_of(t), range(1, last), blocks, lane, {}, {}))
        return carry

    lax.fori_loop(1, strips - 1, interior, 0)

    @pl.when(has_north)
    def _():
        for copy in south_copies:
            copy.wait_recv()

    @pl.when(has_south)
    def _():
        for copy in north_copies:
            copy.wait_recv()

    def merge(t, carry):
        rows = pl.ds(pl.multiple_of(PAD - SUB + t * SUB, SUB), SUB)
        x[inner, rows, :] = jnp.where(lane < LANES // 2, e[1, rows, :], e[0, rows, :])
        return carry

    lax.fori_loop(0, strips + 2, merge, 0)
    each_gather(lambda copy: copy.wait_recv())

    @pl.when(pole)
    def _():
        summed = lax.fori_loop(1, n_lon, lambda d, total: total + gat[d], gat[0])
        k = jnp.where(lat == 0, lane, LANES - 1 - lane)
        third = jnp.where(k < 3, 1.0 / 3.0, 0.0)
        both = third + jnp.where(k < 4, 0.25, 0.0) + jnp.where(k < 5, 0.2, 0.0)
        around = float(cols * n_lon)
        near = jnp.where(k < 5, summed, 0.0)
        means[0] = jnp.full((SUB, LANES), jnp.sum(near * third) / around, jnp.float32)
        means[1] = jnp.full((SUB, LANES), jnp.sum(near * both) / (3.0 * around), jnp.float32)

    @pl.when(jnp.logical_not(pole))
    def _():
        means[...] = jnp.zeros(means.shape, jnp.float32)

    scale, extra = edge_factors(blocks, rows_here, total_rows, lat * rows_here, lane, means[0])

    def sides(t, carry):
        run(box_strip(x, z1, row_of(t), (last, inner, 0), blocks, lane, scale, extra))
        return carry

    lax.fori_loop(1, strips - 1, sides, 0)
    for copy in lon_copies:
        copy.wait_recv()
    whole = list(range(blocks))

    def ends(t, carry):
        strip = t + (t // 2) * (strips - 2)
        row = pl.multiple_of(PAD - SUB + strip * SUB, SUB)
        run(box_strip(x, z1, row, whole, blocks, lane, scale, extra))
        return carry

    lax.fori_loop(0, 4, ends, 0)

    for copy in lon_copies:
        copy.wait_send()

    @pl.when(has_south)
    def _():
        for copy in south_copies:
            copy.wait_send()

    @pl.when(has_north)
    def _():
        for copy in north_copies:
            copy.wait_send()

    each_gather(lambda copy: copy.wait_send())


def second_kernel(n_lat, cols, rows_here, chunk, z1, means, stretch, smooth_hbm, slope_hbm, z2, smooth, slope, sem):
    inner = rows_here // LANES
    blocks = inner + 1
    lat = lax.axis_index("lat")
    lane = lax.broadcasted_iota(jnp.int32, (SUB, LANES), 1)
    scale, extra = edge_factors(
        blocks, rows_here, rows_here * n_lat, lat * rows_here, lane, means[1]
    )
    whole = [inner] + list(range(inner))
    strips = cols // SUB

    def row_of(t):
        return pl.multiple_of(PAD + t * SUB, SUB)

    def smooth_strip(t, keep):
        for b, value in box_strip(z1, z2, row_of(t), whole, blocks, lane, scale, extra):
            if keep and b < inner:
                smooth[pl.ds(pl.multiple_of(t * SUB, SUB), SUB), b * LANES : (b + 1) * LANES] = value

    def slope_strip(t):
        row = row_of(t)

        def rows(b):
            return [z2[b, pl.ds(row + d, SUB), :] for d in (-1, 0, 1)]

        loaded = Strip(blocks, rows)
        across = Strip(blocks, lambda b: loaded[b][2] - loaded[b][0])
        pair = Strip(blocks, lambda b: across[b] + across.ahead(b, 1, lane))
        weighted = Strip(blocks, lambda b: (loaded[b][0] + loaded[b][2]) + (loaded[b][1] + loaded[b][1]))
        for b in range(inner):
            east_west = pair[b] + pair.ahead(b, -1, lane)
            north_south = weighted.ahead(b, 1, lane) - weighted.ahead(b, -1, lane)
            gx = east_west * stretch[pl.ds(b, 1), :]
            gy = north_south * 0.125
            q = 1.0 + gx * gx + gy * gy
            slope[pl.ds(pl.multiple_of(t * SUB, SUB), SUB), b * LANES : (b + 1) * LANES] = q * lax.rsqrt(q)

    smooth_strip(-1, False)
    smooth_strip(0, True)
    smooth_strip(strips, False)
    copies = []
    done = 0
    for c in range(strips // chunk):
        first, end = c * chunk, (c + 1) * chunk

        def both(t, carry):
            smooth_strip(t + 1, True)
            slope_strip(t)
            return carry

        lax.fori_loop(first, min(end, strips - 1), both, 0)
        if end == strips:
            slope_strip(strips - 1)
        rows = pl.ds(first * SUB, chunk * SUB)
        for i, (src, dst) in enumerate(((smooth, smooth_hbm), (slope, slope_hbm))):
            copy = pltpu.make_async_copy(src.at[rows, :], dst.at[0, rows, :], sem.at[i, c])
            copy.start()
            copies.append(copy)
    for copy in copies:
        copy.wait()


def divisor(count, most):
    return max(d for d in range(1, most + 1) if count % d == 0)


def solution(mesh):
    n_lon, n_lat = mesh.shape["lon"], mesh.shape["lat"]

    def local(terrain_relief):
        _, cols, rows_here = terrain_relief.shape
        inner = rows_here // LANES
        blocks = inner + 1
        tall = cols + 2 * PAD
        f32 = jnp.float32
        start = lax.axis_index("lat") * rows_here
        row = (start + jnp.arange(rows_here, dtype=jnp.int32)).astype(f32)
        latitude = jnp.pi * ((row + 0.5) / (rows_here * n_lat) - 0.5)
        stretch = 0.125 / jnp.maximum(jnp.cos(latitude), 0.1)
        stretch = stretch.reshape(inner, LANES)
        vmem = pl.BlockSpec(memory_space=pltpu.VMEM)
        hbm = pl.BlockSpec(memory_space=pltpu.HBM)
        z1, means = pl.pallas_call(
            functools.partial(first_kernel, n_lon, n_lat, cols, rows_here),
            out_shape=(
                jax.ShapeDtypeStruct((blocks, tall, LANES), f32),
                jax.ShapeDtypeStruct((2, SUB, LANES), f32),
            ),
            in_specs=[hbm],
            out_specs=(vmem, vmem),
            scratch_shapes=[
                pltpu.VMEM((blocks, tall, LANES), f32),
                pltpu.VMEM((2, tall, LANES), f32),
                pltpu.VMEM((n_lon, SUB, LANES), f32),
                pltpu.SemaphoreType.DMA((inner,)),
                pltpu.SemaphoreType.DMA((8,)),
                pltpu.SemaphoreType.DMA((8,)),
                pltpu.SemaphoreType.DMA((n_lon,)),
                pltpu.SemaphoreType.DMA((n_lon,)),
            ],
            compiler_params=pltpu.CompilerParams(
                collective_id=0, has_side_effects=True, vmem_limit_bytes=24 * 2**20
            ),
        )(terrain_relief)
        chunk = divisor(cols // SUB, 7)
        return pl.pallas_call(
            functools.partial(second_kernel, n_lat, cols, rows_here, chunk),
            out_shape=(jax.ShapeDtypeStruct(terrain_relief.shape, f32),) * 2,
            in_specs=[vmem, vmem, vmem],
            out_specs=(hbm, hbm),
            scratch_shapes=[
                pltpu.VMEM((blocks, tall, LANES), f32),
                pltpu.VMEM((cols, rows_here), f32),
                pltpu.VMEM((cols, rows_here), f32),
                pltpu.SemaphoreType.DMA((2, cols // SUB // chunk)),
            ],
            compiler_params=pltpu.CompilerParams(vmem_limit_bytes=24 * 2**20),
        )(z1, means, stretch)

    return jax.shard_map(
        local,
        mesh=mesh,
        in_specs=(P(None, "lon", "lat"),),
        out_specs=(P(None, "lon", "lat"), P(None, "lon", "lat")),
        check_vma=False,
    )
```

```python
import functools

import jax
import jax.numpy as jnp
from jax import lax
from jax.experimental import pallas as pl
from jax.experimental.pallas import tpu as pltpu
from jax.sharding import PartitionSpec as P

LANES = 128
SUB = 8
PAD = 16
HIGH = 16
MARGIN = 5


class Strip:
    def __init__(self, count, make):
        self.count, self.make = count, make
        self.values, self.rolled = {}, {}

    def __getitem__(self, block):
        block %= self.count
        if block not in self.values:
            self.values[block] = self.make(block)
        return self.values[block]

    def roll(self, block, shift):
        key = (block % self.count, shift)
        if key not in self.rolled:
            self.rolled[key] = pltpu.roll(self[block], (-shift) % LANES, 1)
        return self.rolled[key]

    def ahead(self, block, shift, lane):
        if shift > 0:
            return jnp.where(lane < LANES - shift, self.roll(block, shift), self.roll(block + 1, shift))
        return jnp.where(lane >= -shift, self.roll(block, shift), self.roll(block - 1, shift))


def box_strip(src, dst, row, blocks, total_blocks, lane, scale, extra):
    def lon_sum(b):
        rows = [src[b, pl.ds(row + d, HIGH), :] for d in (-2, -1, 0, 1, 2)]
        return ((rows[0] + rows[1]) + (rows[3] + rows[4])) + rows[2]

    one = Strip(total_blocks, lon_sum)
    two = Strip(total_blocks, lambda b: one[b] + one.ahead(b, 1, lane))
    for b in blocks:
        total = (two[b] + two.ahead(b, -2, lane)) + one.ahead(b, 2, lane)
        if b in scale:
            value = total * scale[b] + extra[b]
        else:
            value = total * (1.0 / 25.0)
        dst[b, pl.ds(row, HIGH), :] = value
        yield b, value


def run(strip):
    for _ in strip:
        pass


def edge_rows(blocks, rows_here, start, lane):
    inner = blocks - 1
    return {
        0: start + lane,
        inner - 1: start + rows_here - LANES + lane,
        inner: jnp.where(lane < LANES // 2, start + rows_here + lane, start - LANES + lane),
    }


def edge_factors(blocks, rows_here, total_rows, start, lane, mean):
    scale, extra = {}, {}
    for b, row in edge_rows(blocks, rows_here, start, lane).items():
        low = jnp.maximum(row - 2, 0)
        high = jnp.minimum(row + 2, total_rows - 1)
        counted = jnp.maximum(high - low + 1, 1).astype(jnp.float32)
        polar = (row == 0) | (row == total_rows - 1)
        inside = (row > 0) & (row < total_rows - 1)
        tiles = HIGH // SUB
        scale[b] = jnp.concatenate([jnp.where(inside, 1.0 / (5.0 * counted), 0.0)] * tiles, 0)
        extra[b] = jnp.concatenate([jnp.where(polar, mean, 0.0)] * tiles, 0)
    return scale, extra


def first_kernel(n_lon, n_lat, cols, rows_here, x_hbm, z1, means, x, e, gat, in_sem, send, recv, gsend, grecv):
    inner = rows_here // LANES
    blocks = inner + 1
    lon, lat = lax.axis_index("lon"), lax.axis_index("lat")
    total_rows = rows_here * n_lat
    east, west = lax.rem(lon + 1, n_lon), lax.rem(lon + n_lon - 1, n_lon)
    has_north, has_south = lat > 0, lat < n_lat - 1
    pole = jnp.logical_not(has_north & has_south)
    lane = lax.broadcasted_iota(jnp.int32, (SUB, LANES), 1)
    wide = lax.broadcasted_iota(jnp.int32, (HIGH, LANES), 1)

    loads = [
        pltpu.make_async_copy(
            x_hbm.at[0, :, pl.ds(b * LANES, LANES)], x.at[b, pl.ds(PAD, cols), :], in_sem.at[b]
        )
        for b in range(inner)
    ]
    for b in [0, inner - 1] + list(range(1, inner - 1)):
        loads[b].start()

    barrier = pltpu.get_barrier_semaphore()

    def greet(to_lon, to_lat):
        pl.semaphore_signal(
            barrier, inc=1, device_id=(to_lon, to_lat), device_id_type=pl.DeviceIdType.MESH
        )

    greet(east, lat)
    greet(west, lat)

    @pl.when(has_north)
    def _():
        for to_lon in (lon, east, west):
            greet(to_lon, lat - 1)

    @pl.when(has_south)
    def _():
        for to_lon in (lon, east, west):
            greet(to_lon, lat + 1)

    @pl.when(pole)
    def _():
        def one(d, carry):
            greet(lax.rem(lon + d, n_lon), lat)
            return carry

        lax.fori_loop(2, n_lon - 1, one, 0)

    def remote(src, dst, i, to_lon, to_lat):
        return pltpu.make_async_remote_copy(
            src_ref=src,
            dst_ref=dst,
            send_sem=send.at[i],
            recv_sem=recv.at[i],
            device_id=(to_lon, to_lat),
            device_id_type=pl.DeviceIdType.MESH,
        )

    own = pl.ds(PAD, cols)
    head, tail = pl.ds(PAD, MARGIN), pl.ds(PAD + cols - MARGIN, MARGIN)
    before, after = pl.ds(PAD - MARGIN, MARGIN), pl.ds(PAD + cols, MARGIN)
    band = pl.ds(0, inner)
    last = inner - 1
    lon_copies = [
        remote(x.at[band, tail, :], x.at[band, before, :], 0, east, lat),
        remote(x.at[band, head, :], x.at[band, after, :], 1, west, lat),
    ]
    south_copies = [
        remote(x.at[last, own, :], e.at[0, own, :], 2, lon, lat + 1),
        remote(x.at[last, tail, :], e.at[0, before, :], 3, east, lat + 1),
        remote(x.at[last, head, :], e.at[0, after, :], 4, west, lat + 1),
    ]
    north_copies = [
        remote(x.at[0, own, :], e.at[1, own, :], 5, lon, lat - 1),
        remote(x.at[0, tail, :], e.at[1, before, :], 6, east, lat - 1),
        remote(x.at[0, head, :], e.at[1, after, :], 7, west, lat - 1),
    ]

    def gather_copy(d):
        return pltpu.make_async_remote_copy(
            src_ref=gat.at[0],
            dst_ref=gat.at[d],
            send_sem=gsend.at[d],
            recv_sem=grecv.at[d],
            device_id=(lax.rem(lon + d, n_lon), lat),
            device_id_type=pl.DeviceIdType.MESH,
        )

    loads[0].wait()
    loads[last].wait()

    def partial_sum(block):
        def one(t, total):
            return total + x[block, pl.ds(pl.multiple_of(PAD + t * SUB, SUB), SUB), :]

        gat[0] = lax.fori_loop(0, cols // SUB, one, jnp.zeros((SUB, LANES), jnp.float32), unroll=True)

    pl.when(lat == 0)(lambda: partial_sum(0))
    pl.when(lat == n_lat - 1)(lambda: partial_sum(last))

    signals = 2 + 3 * has_north.astype(jnp.int32) + 3 * has_south.astype(jnp.int32)
    signals = signals + (n_lon - 3) * pole.astype(jnp.int32)
    pl.semaphore_wait(barrier, signals)

    @pl.when(has_south)
    def _():
        for copy in south_copies:
            copy.start()

    @pl.when(has_north)
    def _():
        for copy in north_copies:
            copy.start()

    for b in range(1, last):
        loads[b].wait()
    for copy in lon_copies:
        copy.start()

    def each_gather(act):
        @pl.when(pole)
        def _():
            def one(d, carry):
                act(gather_copy(d))
                return carry

            lax.fori_loop(1, n_lon, one, 0)

    each_gather(lambda copy: copy.start())

    def clear(side):
        e[side] = jnp.zeros(e.shape[1:], jnp.float32)

    pl.when(jnp.logical_not(has_north))(lambda: clear(0))
    pl.when(jnp.logical_not(has_south))(lambda: clear(1))

    strips = cols // SUB

    def row_of(t):
        return pl.multiple_of(PAD + SUB + t * HIGH, SUB)

    middle = (cols - 2 * SUB) // HIGH

    def interior(t, carry):
        run(box_strip(x, z1, row_of(t), range(1, last), blocks, wide, {}, {}))
        return carry

    lax.fori_loop(0, middle, interior, 0)

    @pl.when(has_north)
    def _():
        for copy in south_copies:
            copy.wait_recv()

    @pl.when(has_south)
    def _():
        for copy in north_copies:
            copy.wait_recv()

    def merge(t, carry):
        rows = pl.ds(pl.multiple_of(PAD - SUB + t * SUB, SUB), SUB)
        x[inner, rows, :] = jnp.where(lane < LANES // 2, e[1, rows, :], e[0, rows, :])
        return carry

    lax.fori_loop(0, strips + 2, merge, 0)
    each_gather(lambda copy: copy.wait_recv())

    @pl.when(pole)
    def _():
        summed = lax.fori_loop(1, n_lon, lambda d, total: total + gat[d], gat[0])
        k = jnp.where(lat == 0, lane, LANES - 1 - lane)
        third = jnp.where(k < 3, 1.0 / 3.0, 0.0)
        both = third + jnp.where(k < 4, 0.25, 0.0) + jnp.where(k < 5, 0.2, 0.0)
        around = float(cols * n_lon)
        near = jnp.where(k < 5, summed, 0.0)
        means[0] = jnp.full((SUB, LANES), jnp.sum(near * third) / around, jnp.float32)
        means[1] = jnp.full((SUB, LANES), jnp.sum(near * both) / (3.0 * around), jnp.float32)

    @pl.when(jnp.logical_not(pole))
    def _():
        means[...] = jnp.zeros(means.shape, jnp.float32)

    scale, extra = edge_factors(blocks, rows_here, total_rows, lat * rows_here, lane, means[0])

    def sides(t, carry):
        run(box_strip(x, z1, row_of(t), (last, inner, 0), blocks, wide, scale, extra))
        return carry

    lax.fori_loop(0, middle, sides, 0, unroll=2)
    for copy in lon_copies:
        copy.wait_recv()
    whole = list(range(blocks))

    def ends(t, carry):
        row = pl.multiple_of(PAD - SUB + t * cols, SUB)
        run(box_strip(x, z1, row, whole, blocks, wide, scale, extra))
        return carry

    lax.fori_loop(0, 2, ends, 0)

    for copy in lon_copies:
        copy.wait_send()

    @pl.when(has_south)
    def _():
        for copy in south_copies:
            copy.wait_send()

    @pl.when(has_north)
    def _():
        for copy in north_copies:
            copy.wait_send()

    each_gather(lambda copy: copy.wait_send())


def second_kernel(n_lat, cols, rows_here, chunk, z1, means, stretch, smooth_hbm, slope_hbm, z2, smooth, slope, sem):
    inner = rows_here // LANES
    blocks = inner + 1
    lat = lax.axis_index("lat")
    lane = lax.broadcasted_iota(jnp.int32, (SUB, LANES), 1)
    wide = lax.broadcasted_iota(jnp.int32, (HIGH, LANES), 1)
    scale, extra = edge_factors(
        blocks, rows_here, rows_here * n_lat, lat * rows_here, lane, means[1]
    )
    whole = [inner] + list(range(inner))
    strips = cols // HIGH

    def smooth_strip(row, out_row):
        for b, value in box_strip(z1, z2, row, whole, blocks, wide, scale, extra):
            if b < inner:
                smooth[pl.ds(out_row, HIGH), b * LANES : (b + 1) * LANES] = value

    def slope_strip(row, out_row):
        def rows(b):
            return [z2[b, pl.ds(row + d, HIGH), :] for d in (-1, 0, 1)]

        loaded = Strip(blocks, rows)
        across = Strip(blocks, lambda b: loaded[b][2] - loaded[b][0])
        pair = Strip(blocks, lambda b: across[b] + across.ahead(b, 1, wide))
        weighted = Strip(blocks, lambda b: (loaded[b][0] + loaded[b][2]) + (loaded[b][1] + loaded[b][1]))
        for b in range(inner):
            east_west = pair[b] + pair.ahead(b, -1, wide)
            north_south = weighted.ahead(b, 1, wide) - weighted.ahead(b, -1, wide)
            gx = east_west * stretch[pl.ds(b, 1), :]
            gy = north_south * 0.125
            q = 1.0 + gx * gx + gy * gy
            slope[pl.ds(out_row, HIGH), b * LANES : (b + 1) * LANES] = q * lax.rsqrt(q)

    def copies(c):
        start = pl.multiple_of(c * (chunk * HIGH), SUB)
        rows = pl.ds(start, chunk * HIGH)
        return [
            pltpu.make_async_copy(
                src.at[pl.ds(start + lead, chunk * HIGH), :], dst.at[0, rows, :], sem.at[i, c]
            )
            for i, (src, dst, lead) in enumerate(
                ((smooth, smooth_hbm, SUB), (slope, slope_hbm, 2 * HIGH))
            )
        ]

    def step(u, carry):
        out_row = pl.multiple_of(u * HIGH, SUB)
        slope_strip(pl.multiple_of(PAD + jnp.maximum(u - 2, 0) * HIGH, SUB), out_row)
        smooth_strip(pl.multiple_of(PAD - SUB + jnp.minimum(u, strips) * HIGH, SUB), out_row)

        @pl.when((u > 2) & (lax.rem(u + chunk - 1, chunk) == 0))
        def _():
            for copy in copies(jnp.maximum(u - 1, chunk) // chunk - 1):
                copy.start()

        return carry

    lax.fori_loop(0, strips + 2, step, 0)

    def finish(c, carry):
        for copy in copies(c):
            copy.wait()
        return carry

    lax.fori_loop(0, strips // chunk, finish, 0)


def divisor(count, most):
    return max(d for d in range(1, most + 1) if count % d == 0)


def solution(mesh):
    n_lon, n_lat = mesh.shape["lon"], mesh.shape["lat"]

    def local(terrain_relief):
        _, cols, rows_here = terrain_relief.shape
        inner = rows_here // LANES
        blocks = inner + 1
        tall = cols + 2 * PAD
        f32 = jnp.float32
        start = lax.axis_index("lat") * rows_here
        row = (start + jnp.arange(rows_here, dtype=jnp.int32)).astype(f32)
        latitude = jnp.pi * ((row + 0.5) / (rows_here * n_lat) - 0.5)
        stretch = 0.125 / jnp.maximum(jnp.cos(latitude), 0.1)
        stretch = stretch.reshape(inner, LANES)
        vmem = pl.BlockSpec(memory_space=pltpu.VMEM)
        hbm = pl.BlockSpec(memory_space=pltpu.HBM)
        z1, means = pl.pallas_call(
            functools.partial(first_kernel, n_lon, n_lat, cols, rows_here),
            out_shape=(
                pltpu.VMEM((blocks, tall, LANES), f32),
                pltpu.VMEM((2, SUB, LANES), f32),
            ),
            in_specs=[hbm],
            out_specs=(vmem, vmem),
            scratch_shapes=[
                pltpu.VMEM((blocks, tall, LANES), f32),
                pltpu.VMEM((2, tall, LANES), f32),
                pltpu.VMEM((n_lon, SUB, LANES), f32),
                pltpu.SemaphoreType.DMA((inner,)),
                pltpu.SemaphoreType.DMA((8,)),
                pltpu.SemaphoreType.DMA((8,)),
                pltpu.SemaphoreType.DMA((n_lon,)),
                pltpu.SemaphoreType.DMA((n_lon,)),
            ],
            compiler_params=pltpu.CompilerParams(
                collective_id=0, has_side_effects=True, vmem_limit_bytes=54 * 2**20
            ),
        )(terrain_relief)
        chunk = divisor(cols // HIGH, 4)
        return pl.pallas_call(
            functools.partial(second_kernel, n_lat, cols, rows_here, chunk),
            out_shape=(jax.ShapeDtypeStruct(terrain_relief.shape, f32),) * 2,
            in_specs=[vmem, vmem, vmem],
            out_specs=(hbm, hbm),
            scratch_shapes=[
                pltpu.VMEM((blocks, tall, LANES), f32),
                pltpu.VMEM((tall, rows_here), f32),
                pltpu.VMEM((tall, rows_here), f32),
                pltpu.SemaphoreType.DMA((2, cols // HIGH // chunk)),
            ],
            compiler_params=pltpu.CompilerParams(vmem_limit_bytes=24 * 2**20),
        )(z1, means, stretch)

    return jax.shard_map(
        local,
        mesh=mesh,
        in_specs=(P(None, "lon", "lat"),),
        out_specs=(P(None, "lon", "lat"), P(None, "lon", "lat")),
        check_vma=False,
    )
```

```python
import functools

import jax
import jax.numpy as jnp
from jax import lax
from jax.experimental import pallas as pl
from jax.experimental.pallas import tpu as pltpu
from jax.sharding import PartitionSpec as P

LANES = 128
SUB = 8
PAD = 16
HIGH = 16
STEP = 8
MARGIN = 5


class Strip:
    def __init__(self, count, make):
        self.count, self.make = count, make
        self.values, self.rolled = {}, {}

    def __getitem__(self, block):
        block %= self.count
        if block not in self.values:
            self.values[block] = self.make(block)
        return self.values[block]

    def roll(self, block, shift):
        key = (block % self.count, shift)
        if key not in self.rolled:
            self.rolled[key] = pltpu.roll(self[block], (-shift) % LANES, 1)
        return self.rolled[key]

    def ahead(self, block, shift, lane):
        if shift > 0:
            return jnp.where(lane < LANES - shift, self.roll(block, shift), self.roll(block + 1, shift))
        return jnp.where(lane >= -shift, self.roll(block, shift), self.roll(block - 1, shift))


def box_strip(src, dst, row, blocks, total_blocks, lane, scale, extra):
    high = lane.shape[0]

    def lon_sum(b):
        rows = [src[b, pl.ds(row + d, high), :] for d in (-2, -1, 0, 1, 2)]
        return ((rows[0] + rows[1]) + (rows[3] + rows[4])) + rows[2]

    one = Strip(total_blocks, lon_sum)
    two = Strip(total_blocks, lambda b: one[b] + one.ahead(b, 1, lane))
    for b in blocks:
        total = (two[b] + two.ahead(b, -2, lane)) + one.ahead(b, 2, lane)
        if b in scale:
            value = total * scale[b] + extra[b]
        else:
            value = total * (1.0 / 25.0)
        dst[b, pl.ds(row, high), :] = value
        yield b, value


def run(strip):
    for _ in strip:
        pass


def edge_rows(blocks, rows_here, start, lane):
    inner = blocks - 1
    return {
        0: start + lane,
        inner - 1: start + rows_here - LANES + lane,
        inner: jnp.where(lane < LANES // 2, start + rows_here + lane, start - LANES + lane),
    }


def edge_factors(blocks, rows_here, total_rows, start, lane, mean, step):
    scale, extra = {}, {}
    for b, row in edge_rows(blocks, rows_here, start, lane).items():
        low = jnp.maximum(row - 2, 0)
        high = jnp.minimum(row + 2, total_rows - 1)
        counted = jnp.maximum(high - low + 1, 1).astype(jnp.float32)
        polar = (row == 0) | (row == total_rows - 1)
        inside = (row > 0) & (row < total_rows - 1)
        tiles = step // SUB
        scale[b] = jnp.concatenate([jnp.where(inside, 1.0 / (5.0 * counted), 0.0)] * tiles, 0)
        extra[b] = jnp.concatenate([jnp.where(polar, mean, 0.0)] * tiles, 0)
    return scale, extra


def first_kernel(n_lon, n_lat, cols, rows_here, x_hbm, z1, means, x, e, gat, in_sem, send, recv, gsend, grecv):
    inner = rows_here // LANES
    blocks = inner + 1
    lon, lat = lax.axis_index("lon"), lax.axis_index("lat")
    total_rows = rows_here * n_lat
    east, west = lax.rem(lon + 1, n_lon), lax.rem(lon + n_lon - 1, n_lon)
    has_north, has_south = lat > 0, lat < n_lat - 1
    pole = jnp.logical_not(has_north & has_south)
    lane = lax.broadcasted_iota(jnp.int32, (SUB, LANES), 1)
    wide = lax.broadcasted_iota(jnp.int32, (HIGH, LANES), 1)

    loads = [
        pltpu.make_async_copy(
            x_hbm.at[0, :, pl.ds(b * LANES, LANES)], x.at[b, pl.ds(PAD, cols), :], in_sem.at[b]
        )
        for b in range(inner)
    ]
    for b in [0, inner - 1] + list(range(1, inner - 1)):
        loads[b].start()

    barrier = pltpu.get_barrier_semaphore()

    def greet(to_lon, to_lat):
        pl.semaphore_signal(
            barrier, inc=1, device_id=(to_lon, to_lat), device_id_type=pl.DeviceIdType.MESH
        )

    greet(east, lat)
    greet(west, lat)

    @pl.when(has_north)
    def _():
        for to_lon in (lon, east, west):
            greet(to_lon, lat - 1)

    @pl.when(has_south)
    def _():
        for to_lon in (lon, east, west):
            greet(to_lon, lat + 1)

    @pl.when(pole)
    def _():
        def one(d, carry):
            greet(lax.rem(lon + d, n_lon), lat)
            return carry

        lax.fori_loop(2, n_lon - 1, one, 0)

    def remote(src, dst, i, to_lon, to_lat):
        return pltpu.make_async_remote_copy(
            src_ref=src,
            dst_ref=dst,
            send_sem=send.at[i],
            recv_sem=recv.at[i],
            device_id=(to_lon, to_lat),
            device_id_type=pl.DeviceIdType.MESH,
        )

    own = pl.ds(PAD, cols)
    head, tail = pl.ds(PAD, MARGIN), pl.ds(PAD + cols - MARGIN, MARGIN)
    before, after = pl.ds(PAD - MARGIN, MARGIN), pl.ds(PAD + cols, MARGIN)
    band = pl.ds(0, inner)
    last = inner - 1
    lon_copies = [
        remote(x.at[band, tail, :], x.at[band, before, :], 0, east, lat),
        remote(x.at[band, head, :], x.at[band, after, :], 1, west, lat),
    ]
    south_copies = [
        remote(x.at[last, own, :], e.at[0, own, :], 2, lon, lat + 1),
        remote(x.at[last, tail, :], e.at[0, before, :], 3, east, lat + 1),
        remote(x.at[last, head, :], e.at[0, after, :], 4, west, lat + 1),
    ]
    north_copies = [
        remote(x.at[0, own, :], e.at[1, own, :], 5, lon, lat - 1),
        remote(x.at[0, tail, :], e.at[1, before, :], 6, east, lat - 1),
        remote(x.at[0, head, :], e.at[1, after, :], 7, west, lat - 1),
    ]

    def gather_copy(d):
        return pltpu.make_async_remote_copy(
            src_ref=gat.at[0],
            dst_ref=gat.at[d],
            send_sem=gsend.at[d],
            recv_sem=grecv.at[d],
            device_id=(lax.rem(lon + d, n_lon), lat),
            device_id_type=pl.DeviceIdType.MESH,
        )

    loads[0].wait()
    loads[last].wait()

    def partial_sum(block):
        def one(t, total):
            return total + x[block, pl.ds(pl.multiple_of(PAD + t * SUB, SUB), SUB), :]

        gat[0] = lax.fori_loop(0, cols // SUB, one, jnp.zeros((SUB, LANES), jnp.float32), unroll=True)

    pl.when(lat == 0)(lambda: partial_sum(0))
    pl.when(lat == n_lat - 1)(lambda: partial_sum(last))

    signals = 2 + 3 * has_north.astype(jnp.int32) + 3 * has_south.astype(jnp.int32)
    signals = signals + (n_lon - 3) * pole.astype(jnp.int32)
    pl.semaphore_wait(barrier, signals)

    @pl.when(has_south)
    def _():
        for copy in south_copies:
            copy.start()

    @pl.when(has_north)
    def _():
        for copy in north_copies:
            copy.start()

    for b in range(1, last):
        loads[b].wait()
    for copy in lon_copies:
        copy.start()

    def each_gather(act):
        @pl.when(pole)
        def _():
            def one(d, carry):
                act(gather_copy(d))
                return carry

            lax.fori_loop(1, n_lon, one, 0)

    each_gather(lambda copy: copy.start())

    def clear(side):
        e[side] = jnp.zeros(e.shape[1:], jnp.float32)

    pl.when(jnp.logical_not(has_north))(lambda: clear(0))
    pl.when(jnp.logical_not(has_south))(lambda: clear(1))

    strips = cols // SUB

    def row_of(t):
        return pl.multiple_of(PAD + SUB + t * HIGH, SUB)

    middle = (cols - 2 * SUB) // HIGH

    def interior(t, carry):
        run(box_strip(x, z1, row_of(t), range(1, last), blocks, wide, {}, {}))
        return carry

    lax.fori_loop(0, middle, interior, 0)

    @pl.when(has_north)
    def _():
        for copy in south_copies:
            copy.wait_recv()

    @pl.when(has_south)
    def _():
        for copy in north_copies:
            copy.wait_recv()

    def merge(t, carry):
        rows = pl.ds(pl.multiple_of(PAD - SUB + t * SUB, SUB), SUB)
        x[inner, rows, :] = jnp.where(lane < LANES // 2, e[1, rows, :], e[0, rows, :])
        return carry

    lax.fori_loop(0, strips + 2, merge, 0)
    each_gather(lambda copy: copy.wait_recv())

    @pl.when(pole)
    def _():
        summed = lax.fori_loop(1, n_lon, lambda d, total: total + gat[d], gat[0])
        k = jnp.where(lat == 0, lane, LANES - 1 - lane)
        third = jnp.where(k < 3, 1.0 / 3.0, 0.0)
        both = third + jnp.where(k < 4, 0.25, 0.0) + jnp.where(k < 5, 0.2, 0.0)
        around = float(cols * n_lon)
        near = jnp.where(k < 5, summed, 0.0)
        means[0] = jnp.full((SUB, LANES), jnp.sum(near * third) / around, jnp.float32)
        means[1] = jnp.full((SUB, LANES), jnp.sum(near * both) / (3.0 * around), jnp.float32)

    @pl.when(jnp.logical_not(pole))
    def _():
        means[...] = jnp.zeros(means.shape, jnp.float32)

    scale, extra = edge_factors(blocks, rows_here, total_rows, lat * rows_here, lane, means[0], HIGH)

    def sides(t, carry):
        run(box_strip(x, z1, row_of(t), (last, inner, 0), blocks, wide, scale, extra))
        return carry

    lax.fori_loop(0, middle, sides, 0, unroll=2)
    for copy in lon_copies:
        copy.wait_recv()
    whole = list(range(blocks))

    def ends(t, carry):
        row = pl.multiple_of(PAD - SUB + t * cols, SUB)
        run(box_strip(x, z1, row, whole, blocks, wide, scale, extra))
        return carry

    lax.fori_loop(0, 2, ends, 0)

    for copy in lon_copies:
        copy.wait_send()

    @pl.when(has_south)
    def _():
        for copy in south_copies:
            copy.wait_send()

    @pl.when(has_north)
    def _():
        for copy in north_copies:
            copy.wait_send()

    each_gather(lambda copy: copy.wait_send())


def second_kernel(n_lat, cols, rows_here, chunk, z1, means, stretch, smooth_hbm, slope_hbm, z2, smooth, slope, sem):
    inner = rows_here // LANES
    blocks = inner + 1
    lat = lax.axis_index("lat")
    lane = lax.broadcasted_iota(jnp.int32, (SUB, LANES), 1)
    wide = lax.broadcasted_iota(jnp.int32, (STEP, LANES), 1)
    scale, extra = edge_factors(
        blocks, rows_here, rows_here * n_lat, lat * rows_here, lane, means[1], STEP
    )
    whole = [inner] + list(range(inner))
    lag = (STEP + 2 * SUB + STEP - 1) // STEP
    strips = (cols + 2 * SUB) // STEP

    def smooth_strip(row, out_row):
        for b, value in box_strip(z1, z2, row, whole, blocks, wide, scale, extra):
            if b < inner:
                smooth[pl.ds(out_row, STEP), b * LANES : (b + 1) * LANES] = value

    def slope_strip(row, out_row):
        def rows(b):
            return [z2[b, pl.ds(row + d, STEP), :] for d in (-1, 0, 1)]

        loaded = Strip(blocks, rows)
        across = Strip(blocks, lambda b: loaded[b][2] - loaded[b][0])
        pair = Strip(blocks, lambda b: across[b] + across.ahead(b, 1, wide))
        weighted = Strip(blocks, lambda b: (loaded[b][0] + loaded[b][2]) + (loaded[b][1] + loaded[b][1]))
        for b in range(inner):
            east_west = pair[b] + pair.ahead(b, -1, wide)
            north_south = weighted.ahead(b, 1, wide) - weighted.ahead(b, -1, wide)
            gx = east_west * stretch[pl.ds(b, 1), :]
            gy = north_south * 0.125
            q = 1.0 + gx * gx + gy * gy
            slope[pl.ds(out_row, STEP), b * LANES : (b + 1) * LANES] = q * lax.rsqrt(q)

    def copies(c):
        start = pl.multiple_of(c * (chunk * STEP), SUB)
        rows = pl.ds(start, chunk * STEP)
        return [
            pltpu.make_async_copy(
                src.at[pl.ds(start + lead, chunk * STEP), :], dst.at[0, rows, :], sem.at[i, c]
            )
            for i, (src, dst, lead) in enumerate(
                ((smooth, smooth_hbm, SUB), (slope, slope_hbm, lag * STEP))
            )
        ]

    def step(u, carry):
        out_row = pl.multiple_of(u * STEP, SUB)
        slope_strip(pl.multiple_of(PAD + jnp.maximum(u - lag, 0) * STEP, SUB), out_row)
        smooth_strip(pl.multiple_of(PAD - SUB + jnp.minimum(u, strips - 1) * STEP, SUB), out_row)

        @pl.when((u >= lag) & (lax.rem(u + 1 + chunk * lag - lag, chunk) == 0))
        def _():
            for copy in copies(jnp.maximum(u + 1 - lag, chunk) // chunk - 1):
                copy.start()

        return carry

    lax.fori_loop(0, cols // STEP + lag, step, 0)

    def finish(c, carry):
        for copy in copies(c):
            copy.wait()
        return carry

    lax.fori_loop(0, cols // STEP // chunk, finish, 0)


def divisor(count, most):
    return max(d for d in range(1, most + 1) if count % d == 0)


def solution(mesh):
    n_lon, n_lat = mesh.shape["lon"], mesh.shape["lat"]

    def local(terrain_relief):
        _, cols, rows_here = terrain_relief.shape
        inner = rows_here // LANES
        blocks = inner + 1
        tall = cols + 2 * PAD
        f32 = jnp.float32
        start = lax.axis_index("lat") * rows_here
        row = (start + jnp.arange(rows_here, dtype=jnp.int32)).astype(f32)
        latitude = jnp.pi * ((row + 0.5) / (rows_here * n_lat) - 0.5)
        stretch = 0.125 / jnp.maximum(jnp.cos(latitude), 0.1)
        stretch = stretch.reshape(inner, LANES)
        vmem = pl.BlockSpec(memory_space=pltpu.VMEM)
        hbm = pl.BlockSpec(memory_space=pltpu.HBM)
        z1, means = pl.pallas_call(
            functools.partial(first_kernel, n_lon, n_lat, cols, rows_here),
            out_shape=(
                pltpu.VMEM((blocks, tall, LANES), f32),
                pltpu.VMEM((2, SUB, LANES), f32),
            ),
            in_specs=[hbm],
            out_specs=(vmem, vmem),
            scratch_shapes=[
                pltpu.VMEM((blocks, tall, LANES), f32),
                pltpu.VMEM((2, tall, LANES), f32),
                pltpu.VMEM((n_lon, SUB, LANES), f32),
                pltpu.SemaphoreType.DMA((inner,)),
                pltpu.SemaphoreType.DMA((8,)),
                pltpu.SemaphoreType.DMA((8,)),
                pltpu.SemaphoreType.DMA((n_lon,)),
                pltpu.SemaphoreType.DMA((n_lon,)),
            ],
            compiler_params=pltpu.CompilerParams(
                collective_id=0, has_side_effects=True, vmem_limit_bytes=54 * 2**20
            ),
        )(terrain_relief)
        chunk = divisor(cols // STEP, 64 // STEP)
        return pl.pallas_call(
            functools.partial(second_kernel, n_lat, cols, rows_here, chunk),
            out_shape=(jax.ShapeDtypeStruct(terrain_relief.shape, f32),) * 2,
            in_specs=[vmem, vmem, vmem],
            out_specs=(hbm, hbm),
            scratch_shapes=[
                pltpu.VMEM((blocks, tall, LANES), f32),
                pltpu.VMEM((tall, rows_here), f32),
                pltpu.VMEM((tall, rows_here), f32),
                pltpu.SemaphoreType.DMA((2, cols // STEP // chunk)),
            ],
            compiler_params=pltpu.CompilerParams(vmem_limit_bytes=24 * 2**20),
        )(z1, means, stretch)

    return jax.shard_map(
        local,
        mesh=mesh,
        in_specs=(P(None, "lon", "lat"),),
        out_specs=(P(None, "lon", "lat"), P(None, "lon", "lat")),
        check_vma=False,
    )
```

```python
import functools

import jax
import jax.numpy as jnp
from jax import lax
from jax.experimental import pallas as pl
from jax.experimental.pallas import tpu as pltpu
from jax.sharding import PartitionSpec as P

LANES = 128
SUB = 8
PAD = 16
HIGH = 16
STEP = 8
MARGIN = 5


class Strip:
    def __init__(self, count, make):
        self.count, self.make = count, make
        self.values, self.rolled = {}, {}

    def __getitem__(self, block):
        block %= self.count
        if block not in self.values:
            self.values[block] = self.make(block)
        return self.values[block]

    def roll(self, block, shift):
        key = (block % self.count, shift)
        if key not in self.rolled:
            self.rolled[key] = pltpu.roll(self[block], (-shift) % LANES, 1)
        return self.rolled[key]

    def ahead(self, block, shift, lane):
        if shift > 0:
            return jnp.where(lane < LANES - shift, self.roll(block, shift), self.roll(block + 1, shift))
        return jnp.where(lane >= -shift, self.roll(block, shift), self.roll(block - 1, shift))


def box_strip(src, dst, row, blocks, total_blocks, lane, scale, extra):
    high = lane.shape[0]

    def lon_sum(b):
        rows = [src[b, pl.ds(row + d, high), :] for d in (-2, -1, 0, 1, 2)]
        return ((rows[0] + rows[1]) + (rows[3] + rows[4])) + rows[2]

    one = Strip(total_blocks, lon_sum)
    two = Strip(total_blocks, lambda b: one[b] + one.ahead(b, 1, lane))
    for b in blocks:
        total = (two[b] + two.ahead(b, -2, lane)) + one.ahead(b, 2, lane)
        if b in scale:
            value = total * scale[b] + extra[b]
        else:
            value = total * (1.0 / 25.0)
        dst[b, pl.ds(row, high), :] = value
        yield b, value


def banded_strip(src, dst, row, high, total_blocks, band, scale, extra):
    def parts(b):
        rows = [src[b, pl.ds(row + d, high), :] for d in (-2, -1, 0, 1, 2)]
        total = ((rows[0] + rows[1]) + (rows[3] + rows[4])) + rows[2]
        large = total.astype(jnp.bfloat16).astype(jnp.float32)
        return jnp.concatenate([large, total - large], 0).astype(jnp.bfloat16)

    split = [parts(b) for b in range(total_blocks)]
    left = jnp.concatenate(
        [
            jnp.concatenate([split[(b + d) % total_blocks] for d in (-1, 0, 1, 2)], 1)
            for b in range(0, total_blocks, 2)
        ],
        0,
    )
    sums = jnp.dot(left, band[...], preferred_element_type=jnp.float32)
    for b in range(total_blocks):
        lanes = slice(b % 2 * LANES, (b % 2 + 1) * LANES)
        first = b // 2 * 2 * high
        total = sums[first : first + high, lanes] + sums[first + high : first + 2 * high, lanes]
        if b in scale:
            value = total * scale[b] + extra[b]
        else:
            value = total * (1.0 / 25.0)
        dst[b, pl.ds(row, high), :] = value
        yield b, value


def run(strip):
    for _ in strip:
        pass


def edge_rows(blocks, rows_here, start, lane):
    inner = blocks - 1
    return {
        0: start + lane,
        inner - 1: start + rows_here - LANES + lane,
        inner: jnp.where(lane < LANES // 2, start + rows_here + lane, start - LANES + lane),
    }


def edge_factors(blocks, rows_here, total_rows, start, lane, mean, step):
    scale, extra = {}, {}
    for b, row in edge_rows(blocks, rows_here, start, lane).items():
        low = jnp.maximum(row - 2, 0)
        high = jnp.minimum(row + 2, total_rows - 1)
        counted = jnp.maximum(high - low + 1, 1).astype(jnp.float32)
        polar = (row == 0) | (row == total_rows - 1)
        inside = (row > 0) & (row < total_rows - 1)
        tiles = step // SUB
        scale[b] = jnp.concatenate([jnp.where(inside, 1.0 / (5.0 * counted), 0.0)] * tiles, 0)
        extra[b] = jnp.concatenate([jnp.where(polar, mean, 0.0)] * tiles, 0)
    return scale, extra


def first_kernel(n_lon, n_lat, cols, rows_here, x_hbm, z1, means, x, e, gat, in_sem, send, recv, gsend, grecv):
    inner = rows_here // LANES
    blocks = inner + 1
    lon, lat = lax.axis_index("lon"), lax.axis_index("lat")
    total_rows = rows_here * n_lat
    east, west = lax.rem(lon + 1, n_lon), lax.rem(lon + n_lon - 1, n_lon)
    has_north, has_south = lat > 0, lat < n_lat - 1
    pole = jnp.logical_not(has_north & has_south)
    lane = lax.broadcasted_iota(jnp.int32, (SUB, LANES), 1)
    wide = lax.broadcasted_iota(jnp.int32, (HIGH, LANES), 1)

    loads = [
        pltpu.make_async_copy(
            x_hbm.at[0, :, pl.ds(b * LANES, LANES)], x.at[b, pl.ds(PAD, cols), :], in_sem.at[b]
        )
        for b in range(inner)
    ]
    for b in [0, inner - 1] + list(range(1, inner - 1)):
        loads[b].start()

    barrier = pltpu.get_barrier_semaphore()

    def greet(to_lon, to_lat):
        pl.semaphore_signal(
            barrier, inc=1, device_id=(to_lon, to_lat), device_id_type=pl.DeviceIdType.MESH
        )

    greet(east, lat)
    greet(west, lat)

    @pl.when(has_north)
    def _():
        for to_lon in (lon, east, west):
            greet(to_lon, lat - 1)

    @pl.when(has_south)
    def _():
        for to_lon in (lon, east, west):
            greet(to_lon, lat + 1)

    @pl.when(pole)
    def _():
        def one(d, carry):
            greet(lax.rem(lon + d, n_lon), lat)
            return carry

        lax.fori_loop(2, n_lon - 1, one, 0)

    def remote(src, dst, i, to_lon, to_lat):
        return pltpu.make_async_remote_copy(
            src_ref=src,
            dst_ref=dst,
            send_sem=send.at[i],
            recv_sem=recv.at[i],
            device_id=(to_lon, to_lat),
            device_id_type=pl.DeviceIdType.MESH,
        )

    own = pl.ds(PAD, cols)
    head, tail = pl.ds(PAD, MARGIN), pl.ds(PAD + cols - MARGIN, MARGIN)
    before, after = pl.ds(PAD - MARGIN, MARGIN), pl.ds(PAD + cols, MARGIN)
    band = pl.ds(0, inner)
    last = inner - 1
    lon_copies = [
        remote(x.at[band, tail, :], x.at[band, before, :], 0, east, lat),
        remote(x.at[band, head, :], x.at[band, after, :], 1, west, lat),
    ]
    south_copies = [
        remote(x.at[last, own, :], e.at[0, own, :], 2, lon, lat + 1),
        remote(x.at[last, tail, :], e.at[0, before, :], 3, east, lat + 1),
        remote(x.at[last, head, :], e.at[0, after, :], 4, west, lat + 1),
    ]
    north_copies = [
        remote(x.at[0, own, :], e.at[1, own, :], 5, lon, lat - 1),
        remote(x.at[0, tail, :], e.at[1, before, :], 6, east, lat - 1),
        remote(x.at[0, head, :], e.at[1, after, :], 7, west, lat - 1),
    ]

    def gather_copy(d):
        return pltpu.make_async_remote_copy(
            src_ref=gat.at[0],
            dst_ref=gat.at[d],
            send_sem=gsend.at[d],
            recv_sem=grecv.at[d],
            device_id=(lax.rem(lon + d, n_lon), lat),
            device_id_type=pl.DeviceIdType.MESH,
        )

    loads[0].wait()
    loads[last].wait()

    def partial_sum(block):
        def one(t, total):
            return total + x[block, pl.ds(pl.multiple_of(PAD + t * SUB, SUB), SUB), :]

        gat[0] = lax.fori_loop(0, cols // SUB, one, jnp.zeros((SUB, LANES), jnp.float32), unroll=True)

    pl.when(lat == 0)(lambda: partial_sum(0))
    pl.when(lat == n_lat - 1)(lambda: partial_sum(last))

    signals = 2 + 3 * has_north.astype(jnp.int32) + 3 * has_south.astype(jnp.int32)
    signals = signals + (n_lon - 3) * pole.astype(jnp.int32)
    pl.semaphore_wait(barrier, signals)

    @pl.when(has_south)
    def _():
        for copy in south_copies:
            copy.start()

    @pl.when(has_north)
    def _():
        for copy in north_copies:
            copy.start()

    for b in range(1, last):
        loads[b].wait()
    for copy in lon_copies:
        copy.start()

    def each_gather(act):
        @pl.when(pole)
        def _():
            def one(d, carry):
                act(gather_copy(d))
                return carry

            lax.fori_loop(1, n_lon, one, 0)

    each_gather(lambda copy: copy.start())

    def clear(side):
        e[side] = jnp.zeros(e.shape[1:], jnp.float32)

    pl.when(jnp.logical_not(has_north))(lambda: clear(0))
    pl.when(jnp.logical_not(has_south))(lambda: clear(1))

    strips = cols // SUB

    def row_of(t):
        return pl.multiple_of(PAD + SUB + t * HIGH, SUB)

    middle = (cols - 2 * SUB) // HIGH

    def interior(t, carry):
        run(box_strip(x, z1, row_of(t), range(1, last), blocks, wide, {}, {}))
        return carry

    lax.fori_loop(0, middle, interior, 0)

    @pl.when(has_north)
    def _():
        for copy in south_copies:
            copy.wait_recv()

    @pl.when(has_south)
    def _():
        for copy in north_copies:
            copy.wait_recv()

    def merge(t, carry):
        rows = pl.ds(pl.multiple_of(PAD - SUB + t * SUB, SUB), SUB)
        x[inner, rows, :] = jnp.where(lane < LANES // 2, e[1, rows, :], e[0, rows, :])
        return carry

    lax.fori_loop(0, strips + 2, merge, 0)
    each_gather(lambda copy: copy.wait_recv())

    @pl.when(pole)
    def _():
        summed = lax.fori_loop(1, n_lon, lambda d, total: total + gat[d], gat[0])
        k = jnp.where(lat == 0, lane, LANES - 1 - lane)
        third = jnp.where(k < 3, 1.0 / 3.0, 0.0)
        both = third + jnp.where(k < 4, 0.25, 0.0) + jnp.where(k < 5, 0.2, 0.0)
        around = float(cols * n_lon)
        near = jnp.where(k < 5, summed, 0.0)
        means[0] = jnp.full((SUB, LANES), jnp.sum(near * third) / around, jnp.float32)
        means[1] = jnp.full((SUB, LANES), jnp.sum(near * both) / (3.0 * around), jnp.float32)

    @pl.when(jnp.logical_not(pole))
    def _():
        means[...] = jnp.zeros(means.shape, jnp.float32)

    scale, extra = edge_factors(blocks, rows_here, total_rows, lat * rows_here, lane, means[0], HIGH)

    def sides(t, carry):
        run(box_strip(x, z1, row_of(t), (last, inner, 0), blocks, wide, scale, extra))
        return carry

    lax.fori_loop(0, middle, sides, 0, unroll=2)
    for copy in lon_copies:
        copy.wait_recv()
    whole = list(range(blocks))

    def ends(t, carry):
        row = pl.multiple_of(PAD - SUB + t * cols, SUB)
        run(box_strip(x, z1, row, whole, blocks, wide, scale, extra))
        return carry

    lax.fori_loop(0, 2, ends, 0)

    for copy in lon_copies:
        copy.wait_send()

    @pl.when(has_south)
    def _():
        for copy in south_copies:
            copy.wait_send()

    @pl.when(has_north)
    def _():
        for copy in north_copies:
            copy.wait_send()

    each_gather(lambda copy: copy.wait_send())


def second_kernel(n_lat, cols, rows_here, chunk, z1, means, stretch, band, smooth_hbm, slope_hbm, z2, smooth, slope, sem):
    inner = rows_here // LANES
    blocks = inner + 1
    lat = lax.axis_index("lat")
    lane = lax.broadcasted_iota(jnp.int32, (SUB, LANES), 1)
    wide = lax.broadcasted_iota(jnp.int32, (STEP, LANES), 1)
    scale, extra = edge_factors(
        blocks, rows_here, rows_here * n_lat, lat * rows_here, lane, means[1], STEP
    )
    lag = (STEP + 2 * SUB + STEP - 1) // STEP
    strips = (cols + 2 * SUB) // STEP

    def smooth_strip(row, out_row):
        for b, value in banded_strip(z1, z2, row, STEP, blocks, band, scale, extra):
            if b < inner:
                smooth[pl.ds(out_row, STEP), b * LANES : (b + 1) * LANES] = value

    def slope_strip(row, out_row):
        def rows(b):
            return [z2[b, pl.ds(row + d, STEP), :] for d in (-1, 0, 1)]

        loaded = Strip(blocks, rows)
        across = Strip(blocks, lambda b: loaded[b][2] - loaded[b][0])
        pair = Strip(blocks, lambda b: across[b] + across.ahead(b, 1, wide))
        weighted = Strip(blocks, lambda b: (loaded[b][0] + loaded[b][2]) + (loaded[b][1] + loaded[b][1]))
        for b in range(inner):
            east_west = pair[b] + pair.ahead(b, -1, wide)
            north_south = weighted.ahead(b, 1, wide) - weighted.ahead(b, -1, wide)
            gx = east_west * stretch[pl.ds(b, 1), :]
            gy = north_south * 0.125
            q = 1.0 + gx * gx + gy * gy
            slope[pl.ds(out_row, STEP), b * LANES : (b + 1) * LANES] = q * lax.rsqrt(q)

    def copies(c):
        start = pl.multiple_of(c * (chunk * STEP), SUB)
        rows = pl.ds(start, chunk * STEP)
        return [
            pltpu.make_async_copy(
                src.at[pl.ds(start + lead, chunk * STEP), :], dst.at[0, rows, :], sem.at[i, c]
            )
            for i, (src, dst, lead) in enumerate(
                ((smooth, smooth_hbm, SUB), (slope, slope_hbm, lag * STEP))
            )
        ]

    def step(u, carry):
        out_row = pl.multiple_of(u * STEP, SUB)
        slope_strip(pl.multiple_of(PAD + jnp.maximum(u - lag, 0) * STEP, SUB), out_row)
        smooth_strip(pl.multiple_of(PAD - SUB + jnp.minimum(u, strips - 1) * STEP, SUB), out_row)

        @pl.when((u >= lag) & (lax.rem(u + 1 + chunk * lag - lag, chunk) == 0))
        def _():
            for copy in copies(jnp.maximum(u + 1 - lag, chunk) // chunk - 1):
                copy.start()

        return carry

    lax.fori_loop(0, cols // STEP + lag, step, 0)

    def finish(c, carry):
        for copy in copies(c):
            copy.wait()
        return carry

    lax.fori_loop(0, cols // STEP // chunk, finish, 0)


def divisor(count, most):
    return max(d for d in range(1, most + 1) if count % d == 0)


def solution(mesh):
    n_lon, n_lat = mesh.shape["lon"], mesh.shape["lat"]

    def local(terrain_relief):
        _, cols, rows_here = terrain_relief.shape
        inner = rows_here // LANES
        blocks = inner + 1
        tall = cols + 2 * PAD
        f32 = jnp.float32
        start = lax.axis_index("lat") * rows_here
        row = (start + jnp.arange(rows_here, dtype=jnp.int32)).astype(f32)
        latitude = jnp.pi * ((row + 0.5) / (rows_here * n_lat) - 0.5)
        stretch = 0.125 / jnp.maximum(jnp.cos(latitude), 0.1)
        stretch = stretch.reshape(inner, LANES)
        offset = jnp.arange(4 * LANES)[:, None] - LANES - jnp.arange(2 * LANES)[None, :]
        band = (jnp.abs(offset) <= 2).astype(jnp.bfloat16)
        vmem = pl.BlockSpec(memory_space=pltpu.VMEM)
        hbm = pl.BlockSpec(memory_space=pltpu.HBM)
        z1, means = pl.pallas_call(
            functools.partial(first_kernel, n_lon, n_lat, cols, rows_here),
            out_shape=(
                pltpu.VMEM((blocks, tall, LANES), f32),
                pltpu.VMEM((2, SUB, LANES), f32),
            ),
            in_specs=[hbm],
            out_specs=(vmem, vmem),
            scratch_shapes=[
                pltpu.VMEM((blocks, tall, LANES), f32),
                pltpu.VMEM((2, tall, LANES), f32),
                pltpu.VMEM((n_lon, SUB, LANES), f32),
                pltpu.SemaphoreType.DMA((inner,)),
                pltpu.SemaphoreType.DMA((8,)),
                pltpu.SemaphoreType.DMA((8,)),
                pltpu.SemaphoreType.DMA((n_lon,)),
                pltpu.SemaphoreType.DMA((n_lon,)),
            ],
            compiler_params=pltpu.CompilerParams(
                collective_id=0, has_side_effects=True, vmem_limit_bytes=54 * 2**20
            ),
        )(terrain_relief)
        chunk = divisor(cols // STEP, 64 // STEP)
        return pl.pallas_call(
            functools.partial(second_kernel, n_lat, cols, rows_here, chunk),
            out_shape=(jax.ShapeDtypeStruct(terrain_relief.shape, f32),) * 2,
            in_specs=[vmem, vmem, vmem, vmem],
            out_specs=(hbm, hbm),
            scratch_shapes=[
                pltpu.VMEM((blocks, tall, LANES), f32),
                pltpu.VMEM((tall, rows_here), f32),
                pltpu.VMEM((tall, rows_here), f32),
                pltpu.SemaphoreType.DMA((2, cols // STEP // chunk)),
            ],
            compiler_params=pltpu.CompilerParams(vmem_limit_bytes=24 * 2**20),
        )(z1, means, stretch, band)

    return jax.shard_map(
        local,
        mesh=mesh,
        in_specs=(P(None, "lon", "lat"),),
        out_specs=(P(None, "lon", "lat"), P(None, "lon", "lat")),
        check_vma=False,
    )
```
